256 devices in a mesh: grp: 32 (over z_hi, y, core), tp: 8 (over z_lo, x).
Axes of the slice: x: 4, y: 4, z: 8 (z_hi: 4, z_lo: 2; z = z_hi * 2 + z_lo), core: 2. Of those that a mesh axis runs over, the one named last changes fastest.
Arguments:
- tokens: bfloat16 [2048, 6144], P('grp', 'tp'), may hold values from -6 to 6
- norm_gain: float32 [6144], replicated, may hold values from 0.25 to 1.75
- router_weight: bfloat16 [6144, 8], replicated, may hold values from -0.078125 to 0.078125
- expert_ids: int32 [2048, 2], P('grp'), may hold values from 0 to 7, all different within a row; in each aligned block of 64 rows (0 to 63, 64 to 127, ...) at most 18 rows name the same one
- gate_proj: bfloat16 [6144, 65536], P(None, ('grp', 'tp')), may hold values from -0.078125 to 0.078125
- up_proj: bfloat16 [6144, 65536], P(None, ('grp', 'tp')), may hold values from -0.078125 to 0.078125
- down_proj: bfloat16 [65536, 6144], P(('grp', 'tp')), may hold values from -0.25 to 0.25
Outputs:
- mixed: bfloat16 [2048, 6144], P('grp', 'tp')
The draws below stay inside these ranges and needn't reach their ends.
Inputs may be any that keep to these rules, and one draw needn't show every extreme that they name: `expert_ids`: each row names two different experts; within the rows of one group (aligned blocks of 64 rows) no expert is named more than 18 times, and in some group one expert is named exactly 18 times.
All inputs are finite; a program needn't handle non-finite values.
Results may differ from the reference program's by a relative error of at most 0.017.
Values may be sent and summed in bfloat16 or wider, within the bound.
A program may use at most 128 MiB of HBM per device.

```python
import math
import jax
import jax.numpy as jnp
import numpy as np
from jax import lax

D = 6144
EXPERTS = 8
FF = 8192
TOK_GRP = 64
CAP = 18
TOKENS = 2048
N_GRP = 32
N_TP = 8


def with_spikes(values, own_key, source, target, blocks, factor):
    def block_of(axis_at):
        return (jnp.arange(values.shape[axis_at]) // (values.shape[axis_at] // blocks)).reshape((-1,) + (1,) * (values.ndim - 1 - axis_at))

    first = jax.random.permutation(own_key, blocks)[block_of(target)]
    far = (block_of(target) + blocks // 2) % blocks
    return jnp.where((block_of(source) == first) | (block_of(source) == far), factor * values, values)


def levels(stream_key, dims, shards, low, top_value):
    def one(axis_at, blocks):
        steps = jax.random.uniform(jax.random.fold_in(jax.random.fold_in(stream_key, 6), axis_at), (blocks,), jnp.float32, low / len(shards), top_value / len(shards))
        return jnp.repeat(jnp.exp(steps), dims[axis_at] // blocks).reshape((-1,) + (1,) * (len(dims) - axis_at - 1))

    factor_of = one(*shards[0])
    for cut in shards[1:]:
        factor_of = factor_of * one(*cut)
    return factor_of


def deal_out(own_key, own, number, rows, amount, top, limit, skew):
    order = jax.random.permutation(own_key, amount)
    crowded, ordinary = shares(amount, rows * top, limit, skew, True), shares(amount, rows * top, limit, skew, False)
    places = jnp.arange(amount)

    def named(sizes, turn):
        used = int((sizes > 0).sum())
        fixed = max(1, used // 4)
        moved = fixed + (places - fixed + turn * (used - fixed)) % max(1, amount - fixed)
        return jnp.zeros((amount,), jnp.int32).at[order[jnp.where(places < fixed, places, moved)]].set(jnp.asarray(sizes, jnp.int32))

    sizes = jnp.where(number % 4 == 0, named(crowded, number // 4), named(ordinary, number - number // 4 - 1))
    mixed = jax.random.permutation(jax.random.fold_in(own, 3), amount)
    giver, sink = mixed[0:amount // 2 * 2:2], mixed[1:amount // 2 * 2:2]
    margin = jnp.minimum(sizes[giver] - 1, limit - sizes[sink]) // 2
    margin = jnp.where((giver == order[0]) | (sink == order[0]) | (sizes[sink] == 0), 0, jnp.maximum(margin, 0))
    moved = jax.random.randint(jax.random.fold_in(own, 4), (amount // 2,), 0, 1 << 20) % (margin + 1)
    sizes = sizes.at[giver].add(-moved).at[sink].add(moved)
    labels = jnp.searchsorted(jnp.cumsum(sizes), jnp.arange(rows * top), side="right").astype(jnp.int32)
    table = labels.reshape(top, rows).T
    table = table[jax.random.permutation(jax.random.fold_in(own, 1), rows)]
    turn = jax.random.randint(jax.random.fold_in(own, 2), (rows, 1), 0, top)
    return jnp.take_along_axis(table, (jnp.arange(top)[None, :] + turn) % top, axis=1)


def shares(amount, total, most, slope, full):
    loads = [(1 << 20) // math.isqrt(standing ** slope) + 1 for standing in range(1, amount + 1)]
    largest = most if full else min(most, max(-(-total // amount), total * loads[0] // sum(loads)))
    least = 1 if total - largest >= amount - 1 else 0
    holding, surplus = [largest] + [least] * (amount - 1), total - largest - least * (amount - 1)
    while surplus > 0:
        candidates = [i for i in range(1, amount) if holding[i] < largest] or [i for i in range(1, amount) if holding[i] < most]
        whole, left = sum([loads[i] for i in candidates]), surplus
        for i in candidates:
            more = min(most - holding[i], max(1, left * loads[i] // whole), surplus)
            holding[i] = holding[i] + more
            surplus = surplus - more
    return np.array(holding)


def gaussian(key, shape, spread, bound, cuts=(), held_as=jnp.bfloat16):
    entries = jax.random.normal(key, shape, jnp.float32) * spread
    if len(cuts) > 0:
        entries = levels(key, shape, cuts, -0.22, 0.18) * entries
    return jnp.clip(entries, min=-bound, max=bound).astype(held_as)


def gaussian_with(rng, extent, width, most, split, heavy, held_as=jnp.bfloat16):
    drawn = width * jax.random.normal(rng, extent, jnp.float32)
    if split:
        drawn = drawn * levels(rng, extent, split, -0.22, 0.18)
    return jnp.clip(with_spikes(drawn, jax.random.fold_in(rng, 3), *heavy), -most, most).astype(held_as)


def setup_inputs(seed: int = 0) -> dict:
    streams_of = jax.random.split(jax.random.key(seed), 8)
    tokens = gaussian(streams_of[0], (TOKENS, D), 1.0, 6.0, ((0, 32), (1, 8)))
    norm_gain = jnp.clip(1.0 + 0.15 * jax.random.normal(streams_of[1], (D,), jnp.float32), 0.25, 1.75)
    router_weight = gaussian(streams_of[2], (D, EXPERTS), D ** -0.5, 0.078125)
    expert_ids_keys = jax.random.split(jax.random.fold_in(streams_of[3], 1), TOKENS // TOK_GRP)
    expert_ids_turns = jax.random.permutation(jax.random.fold_in(streams_of[3], 3), TOKENS // TOK_GRP)
    expert_ids = jax.vmap(lambda own, number: deal_out(jax.random.fold_in(streams_of[3], 2), own, number, TOK_GRP, EXPERTS, 2, CAP, 1))(expert_ids_keys, expert_ids_turns).reshape((TOKENS, 2))
    gate_proj = gaussian(streams_of[4], (D, EXPERTS * FF), D ** -0.5, 0.078125, ((1, 256),))
    up_proj = gaussian(streams_of[5], (D, EXPERTS * FF), D ** -0.5, 0.078125, ((1, 256),))
    down_proj = gaussian_with(streams_of[6], (EXPERTS * FF, D), FF ** -0.5, 0.25, ((0, 256),), (0, 1, 256, 6.0))
    return dict(tokens=tokens, norm_gain=norm_gain, router_weight=router_weight, expert_ids=expert_ids, gate_proj=gate_proj, up_proj=up_proj, down_proj=down_proj)


def reference(tokens, norm_gain, router_weight, expert_ids, gate_proj, up_proj, down_proj):
    epsilon = 1e-05
    values = tokens.astype(jnp.float32)
    mean_square = lax.optimization_barrier(jnp.mean(values * values, axis=-1, keepdims=True))
    normed = (values * lax.rsqrt(mean_square + epsilon) * norm_gain).astype(jnp.bfloat16)
    logits = jnp.dot(normed, router_weight, preferred_element_type=jnp.float32)
    chosen = jnp.take_along_axis(logits, expert_ids, axis=1)
    gate_first = 1.0 / (1.0 + jnp.exp(chosen[:, 1] - chosen[:, 0]))
    gate_second = 1.0 / (1.0 + jnp.exp(chosen[:, 0] - chosen[:, 1]))
    gates = jnp.stack([gate_first, gate_second], axis=1)
    owners = N_GRP // EXPERTS
    slice_width = FF // (owners * N_TP)
    group_ids = expert_ids.reshape(N_GRP, TOK_GRP, 2)
    group_gates = gates.reshape(N_GRP, TOK_GRP, 2)
    mixed = jnp.zeros((TOKENS, D), jnp.float32)
    for expert in range(EXPERTS):
        hits = (group_ids == expert).astype(jnp.int32)
        routed = lax.optimization_barrier(jnp.sum(hits, axis=-1))
        gate_table = lax.optimization_barrier(jnp.sum(group_gates * hits.astype(jnp.float32), axis=-1))
        order = jnp.argsort(1 - routed, axis=1, stable=True)[:, :CAP].astype(jnp.int32)
        valid = jnp.take_along_axis(routed, order, axis=1).astype(jnp.float32)
        token_index = (order + jnp.arange(N_GRP, dtype=jnp.int32)[:, None] * TOK_GRP).reshape(-1)
        row_weight = (jnp.take_along_axis(gate_table, order, axis=1) * valid).reshape(-1)
        row_block = normed[token_index]
        total = jnp.zeros((N_GRP * CAP, D), jnp.float32)
        for quarter in range(owners):
            quarter_sum = jnp.zeros((N_GRP * CAP, D), jnp.float32)
            for piece in range(N_TP):
                column = expert * FF + (quarter * N_TP + piece) * slice_width
                gate_act = jnp.dot(row_block, gate_proj[:, column:column + slice_width], preferred_element_type=jnp.float32)
                up_act = jnp.dot(row_block, up_proj[:, column:column + slice_width], preferred_element_type=jnp.float32)
                hidden = (jax.nn.silu(gate_act) * up_act).astype(jnp.bfloat16)
                partial_out = jnp.dot(hidden, down_proj[column:column + slice_width], preferred_element_type=jnp.float32).astype(jnp.bfloat16)
                quarter_sum = quarter_sum + lax.optimization_barrier(partial_out).astype(jnp.float32)
            total = total + lax.optimization_barrier(quarter_sum.astype(jnp.bfloat16)).astype(jnp.float32)
        mixed = mixed.at[token_index].add(total * row_weight[:, None])
    return mixed.astype(jnp.bfloat16)
```

```python
import functools

import jax
import jax.numpy as jnp
import numpy as np
from jax import lax
from jax.experimental import pallas as pl
from jax.experimental.pallas import tpu as pltpu
from jax.sharding import Mesh
from jax.sharding import PartitionSpec as P

AXES = ("zh", "y", "core", "zl", "x")
GRP = ("zh", "y", "core")
TP = ("zl", "x")
CAP = 18
SLOT = 24
BLOCKS = 8
ROWS = BLOCKS * CAP
EPS = 1e-05
F32 = jnp.float32
BF16 = jnp.bfloat16
MESH = pl.DeviceIdType.MESH

RA, RB, RC, RD = (0, 48), (48, 32), (80, 32), (112, 32)


def rows_of(cut):
    return pl.ds(cut[0], cut[1])


def halves(cut):
    half = cut[1] // 2
    return (cut[0], half), (cut[0] + half, half)


def kernel(
    tokens,
    gain,
    router,
    ids,
    pack,
    gate_hbm,
    up_hbm,
    down_hbm,
    out,
    stats_own,
    stats_in,
    logit_own,
    logit_in,
    sent,
    landed,
    G,
    S,
    Q,
    P1,
    final,
    xa_step1,
    xa_step2,
    a_mid,
    a_last,
    c_far,
    c_mid,
    c_step1,
    c_step2,
    leave,
    back,
    gate_w,
    up_w,
    down_w,
    gate_acc,
    up_acc,
    hidden,
    weight_sem,
    send_sem,
    recv_sem,
):
    zh, y, core = lax.axis_index("zh"), lax.axis_index("y"), lax.axis_index("core")
    zl, x = lax.axis_index("zl"), lax.axis_index("x")
    yi = lax.rem(y, 2)
    pair = lax.div(y, 2)
    piece = zl * 4 + x
    width = tokens.shape[1]
    toks = tokens.shape[0]
    xr, xl, xo = lax.rem(x + 1, 4), lax.rem(x + 3, 4), lax.rem(x + 2, 4)
    y_other, z_other = 1 - yi, 1 - zl
    right, left = {"x": xr}, {"x": xl}
    across_y = {"y": pair * 2 + y_other}
    across_z = {"zl": z_other}
    across_core = {"core": 1 - core}

    peers = []
    for dz in range(2):
        for dx in range(4):
            if dz or dx:
                peers.append({"zl": lax.rem(zl + dz, 2), "x": lax.rem(x + dx, 4)})
    homes = []
    for dz in range(4):
        for k in range(2):
            homes.append({"zh": lax.rem(zh + dz, 4), "y": y if k == 0 else 3 - y})
    sources = []
    for dz in range(4):
        for k in range(2):
            sources.append({"zh": lax.rem(zh + 4 - dz, 4), "y": y if k == 0 else 3 - y})

    barrier = pltpu.get_barrier_semaphore()
    greeted = peers + homes[1:] + [across_y, across_core]
    for who in greeted:
        pl.semaphore_signal(barrier, inc=1, device_id=who, device_id_type=MESH)

    loads = [
        pltpu.make_async_copy(src, dst, weight_sem.at[i])
        for i, (src, dst) in enumerate(((gate_hbm, gate_w), (up_hbm, up_w), (down_hbm, down_w)))
    ]
    for load in loads:
        load.start()

    counter = [0]
    started = []

    def send(src, dst, who):
        i = counter[0]
        counter[0] += 1
        copy = pltpu.make_async_remote_copy(
            src_ref=src,
            dst_ref=dst,
            send_sem=send_sem.at[i],
            recv_sem=recv_sem.at[i],
            device_id=who,
            device_id_type=MESH,
        )
        copy.start()
        started.append(copy)
        return copy

    local = tokens[...].astype(F32)
    column = jnp.sum(local * local, axis=-1, keepdims=True)
    stats_own[...] = jnp.transpose(jnp.broadcast_to(column, (toks, 128)))[0:8, :]
    pl.semaphore_wait(barrier, len(greeted))
    stat_copies = [send(stats_own, stats_in.at[i], who) for i, who in enumerate(peers)]

    sub = lax.broadcasted_iota(jnp.int32, (8, toks), 0)
    expert_of = lax.rem(zh + lax.div(sub, 2), 4) * 2 + lax.rem(pair + lax.rem(sub, 2), 2)
    first = ids[0:1, :] == expert_of
    second = ids[1:2, :] == expert_of
    hit = (first | second).astype(F32)
    upper = (
        lax.broadcasted_iota(jnp.int32, (toks, toks), 0)
        <= lax.broadcasted_iota(jnp.int32, (toks, toks), 1)
    ).astype(F32)
    place = jnp.dot(hit.astype(BF16), upper.astype(BF16), preferred_element_type=F32)
    place = jnp.where(hit > 0.5, place - 1.0, -1.0).astype(jnp.int32)
    slot_iota = lax.broadcasted_iota(jnp.int32, (SLOT, toks), 0)

    for copy in stat_copies:
        copy.wait_recv()
    total = stats_own[...]
    for i in range(len(peers)):
        total = total + stats_in[i]
    scale = lax.rsqrt(total / (8 * width) + EPS)
    scale = jnp.transpose(jnp.broadcast_to(scale[0:1, :], (128, toks)))[:, 0:1]
    gain_part = gain[:, pl.ds(pl.multiple_of(piece * width, 128), width)]
    normed = (tokens[...].astype(F32) * scale * gain_part).astype(BF16)

    for b in range(BLOCKS):
        pick = (place[b : b + 1, :] == slot_iota).astype(F32).astype(BF16)
        rows = jnp.dot(pick, normed, preferred_element_type=F32).astype(BF16)
        if b == 0:
            landed[0] = rows
        else:
            sent[b] = rows
    dispatch = [send(sent.at[b], landed.at[b], homes[b]) for b in range(1, BLOCKS)]

    router_part = router[:, pl.ds(pl.multiple_of(piece * width, 128), width)]
    logit_own[...] = lax.dot_general(
        router_part, normed, (((1,), (1,)), ((), ())), preferred_element_type=F32
    )
    logit_copies = [send(logit_own, logit_in.at[i], who) for i, who in enumerate(peers)]

    for copy in dispatch:
        copy.wait_recv()
    G[0, yi, zl, x] = jnp.dot(
        pack[...],
        landed[...].reshape(BLOCKS * SLOT, width),
        preferred_element_type=F32,
    ).astype(BF16)

    ra, rb, rc, rd = rows_of(RA), rows_of(RB), rows_of(RC), rows_of(RD)
    (c0, c1), (d0, d1) = halves(RC), halves(RD)

    def spread(at, who):
        return send(G.at[at], G.at[at], who)

    a1 = spread((0, yi, zl, x, ra), across_y)
    b1 = spread((0, yi, zl, x, rb), across_z)
    c1p = spread((0, yi, zl, x, rc), right)
    c1m = spread((0, yi, zl, x, rc), left)
    d1p = spread((0, yi, zl, x, rd), right)
    d1m = spread((0, yi, zl, x, rd), left)
    a1.wait_recv()
    a2 = spread((0, slice(None), zl, x, ra), across_z)
    b1.wait_recv()
    b2 = spread((0, yi, slice(None), x, rb), across_y)
    c1p.wait_recv()
    c2p = spread((0, yi, zl, xl, rows_of(c0)), right)
    c1m.wait_recv()
    c2m = spread((0, yi, zl, xr, rows_of(c1)), left)
    d1p.wait_recv()
    d2p = spread((0, yi, zl, xl, rows_of(d0)), right)
    d1m.wait_recv()
    d2m = spread((0, yi, zl, xr, rows_of(d1)), left)
    a2.wait_recv()
    a3p = spread((0, slice(None), slice(None), x, ra), right)
    a3m = spread((0, slice(None), slice(None), x, ra), left)
    b2.wait_recv()
    b3p = spread((0, slice(None), slice(None), x, rb), right)
    b3m = spread((0, slice(None), slice(None), x, rb), left)
    c2p.wait_recv()
    c2m.wait_recv()
    c3 = spread((0, yi, zl, slice(None), rc), across_y)
    d2p.wait_recv()
    d2m.wait_recv()
    d3 = spread((0, yi, zl, slice(None), rd), across_z)
    c3.wait_recv()
    c4 = spread((0, slice(None), zl, slice(None), rc), across_z)
    d3.wait_recv()
    d4 = spread((0, yi, slice(None), slice(None), rd), across_y)
    a3p.wait_recv()
    a4p = spread((0, 0, slice(None), xl, ra), right)
    a3m.wait_recv()
    a4m = spread((0, 1, slice(None), xr, ra), left)
    b3p.wait_recv()
    b4p = spread((0, 0, slice(None), xl, rb), right)
    b3m.wait_recv()
    b4m = spread((0, 1, slice(None), xr, rb), left)
    for copy in (a4p, a4m, b4p, b4m, c4, d4):
        copy.wait_recv()

    cores_in = [
        send(G.at[0, :, p // 4, p % 4], G.at[1, :, p // 4, p % 4], across_core) for p in range(8)
    ]
    loads[0].wait()
    loads[1].wait()

    def half_ff(plane, waits):
        gate_acc[...] = jnp.zeros_like(gate_acc)
        up_acc[...] = jnp.zeros_like(up_acc)

        def step(p):
            at = pl.ds(pl.multiple_of(p * width, 128), width)
            block = G[plane, :, lax.div(p, 4), lax.rem(p, 4)].reshape(2 * ROWS, width)
            gate_acc[...] += jnp.dot(block, gate_w[at, :], preferred_element_type=F32)
            up_acc[...] += jnp.dot(block, up_w[at, :], preferred_element_type=F32)

        if waits is not None:
            for copy in waits:
                copy.wait_recv()
        pl.loop(0, 8)(step)
        act = gate_acc[...]
        hidden[plane] = (act / (1.0 + jnp.exp(-act)) * up_acc[...]).astype(BF16)

    half_ff(0, None)
    half_ff(1, cores_in)
    loads[2].wait()

    def partial_out(plane, p):
        at = pl.ds(pl.multiple_of(p * width, 128), width)
        return jnp.dot(hidden[plane], down_w[:, at], preferred_element_type=F32)

    base = counter[0]
    counter[0] += 8

    def core_copy(p):
        return pltpu.make_async_remote_copy(
            src_ref=P1.at[:, lax.div(p, 4), lax.rem(p, 4)],
            dst_ref=Q.at[:, lax.div(p, 4), lax.rem(p, 4)],
            send_sem=send_sem.at[base + p],
            recv_sem=recv_sem.at[base + p],
            device_id=across_core,
            device_id_type=MESH,
        )

    @pl.loop(0, 8)
    def _(p):
        P1[:, lax.div(p, 4), lax.rem(p, 4)] = (
            partial_out(1, p).astype(BF16).reshape(2, ROWS, width)
        )
        core_copy(p).start()

    @pl.loop(0, 8)
    def _(p):
        product = partial_out(0, p)
        core_copy(p).wait_recv()
        theirs = Q[:, lax.div(p, 4), lax.rem(p, 4)].reshape(2 * ROWS, width)
        S[:, lax.div(p, 4), lax.rem(p, 4)] = (
            (product + theirs.astype(F32)).astype(BF16).reshape(2, ROWS, width)
        )

    def add(dst, src):
        S[dst] = (S[dst].astype(F32) + src.astype(F32)).astype(BF16)

    def a_ops(cut, i):
        n = cut[1]
        r = rows_of(cut)
        at = pl.ds(cut[0], n)
        step1p = send(S.at[0, :, xo, r], xa_step1.at[0, :, at], right)
        step1m = send(S.at[1, :, xo, r], xa_step1.at[1, :, at], left)
        return r, at, step1p, step1m

    ar, aat, a1p, a1m = a_ops(RA, 0)
    br, bat, b1p, b1m = a_ops(RB, 1)
    cc1 = send(S.at[:, z_other, :, rc], c_far.at[0], across_z)
    dd1 = send(S.at[y_other, :, :, rd], c_far.at[1], across_y)

    def x_second(r, at, p1, m1):
        p1.wait_recv()
        for k in range(2):
            add((0, k, xr, r), xa_step1[0, k, at])
        p2 = send(S.at[:, :, xr, r], xa_step2.at[0, :, :, at], right)
        m1.wait_recv()
        for k in range(2):
            add((1, k, xl, r), xa_step1[1, k, at])
        m2 = send(S.at[:, :, xl, r], xa_step2.at[1, :, :, at], left)
        return p2, m2

    a2p, a2m = x_second(ar, aat, a1p, a1m)
    b2p, b2m = x_second(br, bat, b1p, b1m)

    cc1.wait_recv()
    for j in range(2):
        for k in range(4):
            add((j, zl, k, rc), c_far[0, j, k])
    cc2 = send(S.at[y_other, zl, :, rc], c_mid.at[0], across_y)
    dd1.wait_recv()
    for j in range(2):
        for k in range(4):
            add((yi, j, k, rd), c_far[1, j, k])
    dd2 = send(S.at[yi, z_other, :, rd], c_mid.at[1], across_z)

    def x_done(r, at, p2, m2):
        p2.wait_recv()
        m2.wait_recv()
        for j in range(2):
            for k in range(2):
                S[j, k, x, r] = (
                    S[j, k, x, r].astype(F32)
                    + xa_step2[0, j, k, at].astype(F32)
                    + xa_step2[1, j, k, at].astype(F32)
                ).astype(BF16)

    x_done(ar, aat, a2p, a2m)
    a3 = send(S.at[:, z_other, x, ar], a_mid.at[:, aat], across_z)
    x_done(br, bat, b2p, b2m)
    b3 = send(S.at[y_other, :, x, br], a_mid.at[:, bat], across_y)

    def last_x_first(cut, i, mid_copy):
        n = cut[1]
        r = rows_of(cut)
        mid_copy.wait_recv()
        for k in range(4):
            add((yi, zl, k, r), c_mid[i, k])
        lo, hi = halves(cut)
        p1 = send(S.at[yi, zl, xo, rows_of(lo)], c_step1.at[i, 0], right)
        m1 = send(S.at[yi, zl, xo, rows_of(hi)], c_step1.at[i, 1], left)
        return r, lo, hi, p1, m1

    cx = last_x_first(RC, 0, cc2)
    dx = last_x_first(RD, 1, dd2)

    def last_x_second(i, r, lo, hi, p1, m1):
        p1.wait_recv()
        add((yi, zl, xr, rows_of(lo)), c_step1[i, 0])
        p2 = send(S.at[yi, zl, xr, r], c_step2.at[i, 0], right)
        m1.wait_recv()
        add((yi, zl, xl, rows_of(hi)), c_step1[i, 1])
        m2 = send(S.at[yi, zl, xl, r], c_step2.at[i, 1], left)
        return p2, m2

    a3.wait_recv()
    for k in range(2):
        add((k, zl, x, ar), a_mid[k, aat])
    a4 = send(S.at[y_other, zl, x, ar], a_last.at[aat], across_y)
    b3.wait_recv()
    for k in range(2):
        add((yi, k, x, br), a_mid[k, bat])
    b4 = send(S.at[yi, z_other, x, br], a_last.at[bat], across_z)

    cx2 = last_x_second(0, *cx)
    dx2 = last_x_second(1, *dx)

    a4.wait_recv()
    final[ar] = (S[yi, zl, x, ar].astype(F32) + a_last[aat].astype(F32)).astype(BF16)
    b4.wait_recv()
    final[br] = (S[yi, zl, x, br].astype(F32) + a_last[bat].astype(F32)).astype(BF16)
    for i, (r, (p2, m2)) in enumerate(((rc, cx2), (rd, dx2))):
        p2.wait_recv()
        m2.wait_recv()
        final[r] = (
            S[yi, zl, x, r].astype(F32) + c_step2[i, 0].astype(F32) + c_step2[i, 1].astype(F32)
        ).astype(BF16)

    opened = lax.dot_general(
        pack[...], final[...], (((0,), (0,)), ((), ())), preferred_element_type=F32
    ).astype(BF16)
    for b in range(BLOCKS):
        block = opened[b * SLOT : (b + 1) * SLOT]
        if b == 0:
            back[0] = block
        else:
            leave[b] = block
    returns = [send(leave.at[b], back.at[b], sources[b]) for b in range(1, BLOCKS)]

    for copy in logit_copies:
        copy.wait_recv()
    logits = logit_own[...]
    for i in range(len(peers)):
        logits = logits + logit_in[i]
    expert_row = sub
    l0 = jnp.sum(jnp.where(ids[0:1, :] == expert_row, logits, 0.0), axis=0, keepdims=True)
    l1 = jnp.sum(jnp.where(ids[1:2, :] == expert_row, logits, 0.0), axis=0, keepdims=True)
    g0 = 1.0 / (1.0 + jnp.exp(l1 - l0))
    g1 = 1.0 / (1.0 + jnp.exp(l0 - l1))
    share = jnp.where(first, g0, 0.0) + jnp.where(second, g1, 0.0)
    weights = jnp.concatenate(
        [
            jnp.where(place[b : b + 1, :] == slot_iota, share[b : b + 1, :], 0.0)
            for b in range(BLOCKS)
        ],
        axis=0,
    )
    high = weights.astype(BF16)
    low = (weights - high.astype(F32)).astype(BF16)
    for copy in returns:
        copy.wait_recv()
    rows = back[...].reshape(BLOCKS * SLOT, width)
    dims = (((0,), (0,)), ((), ()))
    out[...] = (
        lax.dot_general(high, rows, dims, preferred_element_type=F32)
        + lax.dot_general(low, rows, dims, preferred_element_type=F32)
    ).astype(BF16)

    for copy in started:
        copy.wait_send()

    @pl.loop(0, 8)
    def _(p):
        core_copy(p).wait_send()


def per_device(tokens, norm_gain, router_weight, expert_ids, gate_proj, up_proj, down_proj):
    toks, width = tokens.shape
    hid = gate_proj.shape[1]
    pack = np.zeros((ROWS, BLOCKS * SLOT), np.float32)
    for r in range(ROWS):
        pack[r, r // CAP * SLOT + r % CAP] = 1.0
    vmem = pl.BlockSpec(memory_space=pltpu.VMEM)
    anywhere = pl.BlockSpec(memory_space=pl.ANY)
    n_ab = RA[1] + RB[1]
    n_c = RC[1]
    big = (2, 2, 4, ROWS, width)
    messages = 120
    return pl.pallas_call(
        kernel,
        out_shape=jax.ShapeDtypeStruct((toks, width), BF16),
        in_specs=[vmem] * 5 + [anywhere] * 3,
        out_specs=vmem,
        scratch_shapes=[
            pltpu.VMEM((8, toks), F32),
            pltpu.VMEM((7, 8, toks), F32),
            pltpu.VMEM((8, toks), F32),
            pltpu.VMEM((7, 8, toks), F32),
            pltpu.VMEM((BLOCKS, SLOT, width), BF16),
            pltpu.VMEM((BLOCKS, SLOT, width), BF16),
            pltpu.VMEM((2,) + big, BF16),
            pltpu.VMEM(big, BF16),
            pltpu.VMEM(big, BF16),
            pltpu.VMEM(big, BF16),
            pltpu.VMEM((ROWS, width), BF16),
            pltpu.VMEM((2, 2, n_ab, width), BF16),
            pltpu.VMEM((2, 2, 2, n_ab, width), BF16),
            pltpu.VMEM((2, n_ab, width), BF16),
            pltpu.VMEM((n_ab, width), BF16),
            pltpu.VMEM((2, 2, 4, n_c, width), BF16),
            pltpu.VMEM((2, 4, n_c, width), BF16),
            pltpu.VMEM((2, 2, n_c // 2, width), BF16),
            pltpu.VMEM((2, 2, n_c, width), BF16),
            pltpu.VMEM((BLOCKS, SLOT, width), BF16),
            pltpu.VMEM((BLOCKS, SLOT, width), BF16),
            pltpu.VMEM(gate_proj.shape, BF16),
            pltpu.VMEM(up_proj.shape, BF16),
            pltpu.VMEM(down_proj.shape, BF16),
            pltpu.VMEM((2 * ROWS, hid), F32),
            pltpu.VMEM((2 * ROWS, hid), F32),
            pltpu.VMEM((2, 2 * ROWS, hid), BF16),
            pltpu.SemaphoreType.DMA((3,)),
            pltpu.SemaphoreType.DMA((messages,)),
            pltpu.SemaphoreType.DMA((messages,)),
        ],
        compiler_params=pltpu.CompilerParams(
            collective_id=0, has_side_effects=True, vmem_limit_bytes=63 * 1024 * 1024
        ),
        name="routed_block",
    )(
        tokens,
        norm_gain.reshape(1, -1),
        router_weight.T,
        expert_ids.T,
        jnp.asarray(pack, BF16),
        gate_proj,
        up_proj,
        down_proj,
    )


def solution(mesh):
    split = Mesh(mesh.devices.reshape(4, 4, 2, 2, 4), AXES)
    every = GRP + TP
    placed = (
        P(GRP, TP),
        P(),
        P(),
        P(GRP, None),
        P(None, every),
        P(None, every),
        P(every, None),
    )
    return jax.shard_map(
        per_device, mesh=split, in_specs=placed, out_specs=P(GRP, TP), check_vma=False
    )
```
